32 devices in a mesh: dp: 16 (over z, x, core), head: 2 (over y).
Axes of the slice: x: 2, y: 2, z: 4, core: 2. Of those that a mesh axis runs over, the one named last changes fastest.
Arguments:
- query_clean: float32 [4096, 8192], P(('dp', 'head')), may hold values from -320 to 320
- key_clean: float32 [4096, 1024], P(('dp', 'head')), may hold values from -12 to 12
- clean_value_rows: float32 [4096, 1024], P(('dp', 'head')), may hold values from -6 to 6
- query_corrupt: float32 [4096, 8192], P(('dp', 'head')), may hold values from -320 to 320
- key_corrupt: float32 [4096, 1024], P(('dp', 'head')), may hold values from -12 to 12
- corrupted_value_rows: float32 [4096, 1024], P(('dp', 'head')), may hold values from -6 to 6
- cotangent: float32 [4096, 8192], P(('dp', 'head')), may hold values from -0.3 to 0.3
- bin_segments: int32 [16, 256], P('dp'), may hold values from 0 to 3, never falling along the last dimension, each value on 1 to 128 neighbouring positions
- plan: int32 [16, 16], P('dp'), may hold values from 0 to 15, each once within a row
- offsets: int32 [16], replicated, may hold values from 0 to 15, each once
Outputs:
- head_scores: float32 [64, 64], P('dp', 'head')
- query_scores: float32 [64, 64], P('dp', 'head')
- kv_scores: float32 [64, 8], P('dp', 'head')
The draws below stay inside these ranges and needn't reach their ends.
Inputs may be any that keep to these rules, and one draw needn't show every extreme that they name: `plan`: each row is a permutation of 0 to 15. `offsets`: a permutation: every bin receives exactly one block from each dp index.
All inputs are finite; a program needn't handle non-finite values.
Results may differ from the reference program's by a relative error of at most 0.0003.
Values sent between devices are 32-bit elements; how exact they have to be, the bound alone decides.
No kernel may reach another device: no remote copies, remote signals or barrier semaphores. Data moves between devices by JAX's collectives and lax.ppermute only.
A program may use at most 128 MiB of HBM per device.

```python
import math
import jax
import jax.numpy as jnp
import numpy as np
from jax import lax

QUERY_HEADS = 64
KEY_VALUE_HEADS = 8
HEAD_SIZE = 128
PACK = 256
PAIRS_PER_BIN = 4
NBLK = 16
TOKEN_ROWS_ALL = 4096
N_DP = 16


def query_key(key, salt):
    basis = jax.random.fold_in(key, salt)
    query_random_seed, key_random_seed = jax.random.split(basis, 2)
    key_collections = jnp.clip(jax.random.normal(key_random_seed, (TOKEN_ROWS_ALL, KEY_VALUE_HEADS, HEAD_SIZE), jnp.float32), -6.0, 6.0)
    query_matrix = jnp.clip(jax.random.normal(query_random_seed, (TOKEN_ROWS_ALL, KEY_VALUE_HEADS, QUERY_HEADS // KEY_VALUE_HEADS, HEAD_SIZE), jnp.float32), -6.0, 6.0)
    return (query_matrix.reshape(TOKEN_ROWS_ALL, QUERY_HEADS * HEAD_SIZE), key_collections.reshape(TOKEN_ROWS_ALL, KEY_VALUE_HEADS * HEAD_SIZE))


def draw_query_clean(key, part):
    return query_key(key, 11)[0]


def draw_key_clean(key, part):
    return query_key(key, 11)[1]


def draw_query_corrupt(key, part):
    return query_key(key, 23)[0]


def draw_key_corrupt(key, part):
    return query_key(key, 23)[1]


def block_scale(own_key, shape, cuts, least, largest):
    def one(position, shards_of):
        heights = jax.random.uniform(jax.random.fold_in(jax.random.fold_in(own_key, 6), position), (shards_of,), jnp.float32, least / len(cuts), largest / len(cuts))
        return jnp.repeat(jnp.exp(heights), shape[position] // shards_of).reshape((-1,) + (1,) * (len(shape) - position - 1))

    level = one(*cuts[0])
    for cut in cuts[1:]:
        level = level * one(*cut)
    return level


def profile(number_of, total, limit, slope):
    weights = [(1 << 20) // math.isqrt(standing ** slope) + 1 for standing in range(2, number_of + 1)]
    spare, holding = total - limit - (number_of - 1), [1] * (number_of - 1)
    while spare > 0:
        movable = [i for i in range(number_of - 1) if holding[i] < limit]
        mass, budget = sum([weights[i] for i in movable]), spare
        for i in movable:
            more = min(limit - holding[i], max(1, budget * weights[i] // mass), spare)
            holding[i] = holding[i] + more
            spare = spare - more
    return np.array([limit] + holding)


def ragged(own_key, number_of, total, most, skew):
    if number_of == 2:
        one = jax.random.randint(own_key, (), max(1, total - most), min(most, total - 1) + 1)
        return jnp.stack([one, total - one])
    lengths = jnp.asarray(profile(number_of, total, most, skew), jnp.int32)
    twos = (number_of - 1) // 2
    giver, taker = lengths[1:1 + 2 * twos:2], lengths[2:2 + 2 * twos:2]
    slack = jnp.minimum(giver - 1, most - taker)
    moved = jax.random.randint(jax.random.fold_in(own_key, 1), (twos,), 0, 1 << 20) % (slack + 1)
    lengths = lengths.at[1:1 + 2 * twos:2].set(giver - moved).at[2:2 + 2 * twos:2].set(taker + moved)
    return lengths[jax.random.permutation(jax.random.fold_in(own_key, 2), number_of)]


def gaussian(own_key, shape, scale, most, pieces=(), kind=jnp.bfloat16):
    entries = scale * jax.random.normal(own_key, shape, jnp.float32)
    if pieces:
        entries = entries * block_scale(own_key, shape, pieces, -0.22, 0.18)
    return jnp.clip(entries, -most, most).astype(kind)


def setup_inputs(seed: int = 0) -> dict:
    keys = jax.random.split(jax.random.key(seed), 11)
    query_clean = draw_query_clean(jax.random.fold_in(keys[10], 71), 0)
    key_clean = draw_key_clean(jax.random.fold_in(keys[10], 71), 0)
    clean_value_rows = gaussian(keys[2], (TOKEN_ROWS_ALL, KEY_VALUE_HEADS * HEAD_SIZE), 1.0, 6.0, ((0, 32),), jnp.float32)
    query_corrupt = draw_query_corrupt(jax.random.fold_in(keys[10], 71), 0)
    key_corrupt = draw_key_corrupt(jax.random.fold_in(keys[10], 71), 0)
    corrupted_value_rows = gaussian(keys[5], (TOKEN_ROWS_ALL, KEY_VALUE_HEADS * HEAD_SIZE), 1.0, 6.0, ((0, 32),), jnp.float32)
    cotangent = gaussian(keys[6], (TOKEN_ROWS_ALL, QUERY_HEADS * HEAD_SIZE), 0.05, 0.3, ((0, 32),), jnp.float32)
    bin_segments = jax.vmap(lambda own: jnp.searchsorted(jnp.cumsum(ragged(own, PAIRS_PER_BIN, PACK, PACK // 2, 2)), jnp.arange(PACK), side="right"))(jax.random.split(keys[7], N_DP)).reshape((N_DP, PACK)).astype(jnp.int32)
    plan = jax.vmap(lambda own: jax.random.permutation(own, NBLK))(jax.random.split(keys[8], N_DP)).reshape((N_DP, NBLK)).astype(jnp.int32)
    offsets = jax.random.permutation(keys[9], NBLK).astype(jnp.int32)
    return dict(query_clean=query_clean, key_clean=key_clean, clean_value_rows=clean_value_rows, query_corrupt=query_corrupt, key_corrupt=key_corrupt, corrupted_value_rows=corrupted_value_rows, cotangent=cotangent, bin_segments=bin_segments, plan=plan, offsets=offsets)


TOP_PRECISION = lax.Precision.HIGHEST


def as_views(query_rows, key_rows, value_rows):
    rows_here = query_rows.shape[0]
    width = key_rows.shape[1] // HEAD_SIZE
    groups = query_rows.shape[1] // key_rows.shape[1]
    return (query_rows.reshape(rows_here, width, groups, HEAD_SIZE), key_rows.reshape(rows_here, width, HEAD_SIZE), value_rows.reshape(rows_here, width, HEAD_SIZE))


def attend(query_matrix, key_collections, value_collection, allowed):
    scale_factor = query_matrix.shape[-1] ** -0.5
    score_matrix = jnp.einsum("thxn,whn->hxtw", query_matrix, key_collections, precision=TOP_PRECISION) * scale_factor
    score_matrix = jnp.where(allowed, score_matrix, -jnp.inf)
    peak = jnp.max(score_matrix, axis=-1, keepdims=True)
    raised = jnp.exp(score_matrix - peak)
    weight_matrix = raised / jnp.sum(raised, axis=-1, keepdims=True)
    output_tensors = jnp.einsum("whfo,owj->fwhj", weight_matrix, value_collection, precision=TOP_PRECISION)
    return weight_matrix, output_tensors


def attribute(clean_views, clean_pass, corrupt_views, cotangent, allowed):
    query_matrix, key_collections, value_collection = clean_views
    weight_matrix, output_tensors = clean_pass
    query_other, key_other, value_other = corrupt_views
    scale_factor = query_matrix.shape[-1] ** -0.5
    other_outputs = attend(query_other, key_other, value_other, allowed)[1]
    value_gradient = jnp.einsum("xprv,rxpw->vxw", weight_matrix, cotangent, precision=TOP_PRECISION)
    weight_gradient = jnp.einsum("thxn,whn->hxtw", cotangent, value_collection, precision=TOP_PRECISION)
    row_dot = jnp.transpose(jnp.sum(cotangent * output_tensors, axis=-1), (1, 2, 0))[..., None]
    score_gradient = weight_matrix * (weight_gradient - row_dot) * scale_factor
    query_gradient = jnp.einsum("whfo,owj->fwhj", score_gradient, key_collections, precision=TOP_PRECISION)
    key_gradient = jnp.einsum("xprv,rxpw->vxw", score_gradient, query_matrix, precision=TOP_PRECISION)
    head_terms = jnp.sum((other_outputs - output_tensors) * cotangent, axis=-1)
    query_terms = jnp.sum((query_other - query_matrix) * query_gradient, axis=-1)
    kv_terms = jnp.sum((key_other - key_collections) * key_gradient + (value_other - value_collection) * value_gradient, axis=-1)
    rows_here = query_matrix.shape[0]
    return head_terms.reshape(rows_here, -1), query_terms.reshape(rows_here, -1), kv_terms


def causal_mask(segment_ids):
    row_index = jnp.arange(segment_ids.shape[0], dtype=jnp.int32)
    same = segment_ids[:, None] == segment_ids[None, :]
    return jnp.logical_and(same, row_index[:, None] >= row_index[None, :])


def pair_sums(segment_ids, term_sets):
    members = (segment_ids[:, None] == jnp.arange(PAIRS_PER_BIN, dtype=jnp.int32)[None, :]).astype(jnp.float32)
    return tuple(jnp.dot(members.T, column_set, precision=TOP_PRECISION) for column_set in term_sets)


def reference(query_clean, key_clean, clean_value_rows, query_corrupt, key_corrupt, corrupted_value_rows, cotangent, bin_segments, plan, offsets):
    block_count = offsets.shape[0]
    block_rows = PACK // block_count
    inverse = jnp.zeros((N_DP, block_count), jnp.int32).at[jnp.arange(N_DP, dtype=jnp.int32)[:, None], plan].set(
        jnp.broadcast_to(jnp.arange(block_count, dtype=jnp.int32)[None, :], (N_DP, block_count)))
    arrays = (query_clean, key_clean, clean_value_rows, query_corrupt, key_corrupt, corrupted_value_rows, cotangent)

    def one_bin(bin_index):
        sources = ((bin_index - offsets) % N_DP).astype(jnp.int32)
        which = inverse[sources, jnp.arange(block_count, dtype=jnp.int32)]

        def collect(source_array):
            blocks = source_array.reshape(N_DP, block_count, block_rows, source_array.shape[1])
            return blocks[sources, which].reshape(PACK, source_array.shape[1])

        packed = [collect(source_array) for source_array in arrays]
        segment_ids = bin_segments[bin_index]
        allowed = causal_mask(segment_ids)
        clean_views = as_views(packed[0], packed[1], packed[2])
        corrupt_views = as_views(packed[3], packed[4], packed[5])
        cot_view = packed[6].reshape(clean_views[0].shape)
        clean_pass = attend(clean_views[0], clean_views[1], clean_views[2], allowed)
        term_sets = attribute(clean_views, clean_pass, corrupt_views, cot_view, allowed)
        return pair_sums(segment_ids, term_sets)

    head_portion, query_portion, key_value_portion = lax.map(one_bin, jnp.arange(N_DP, dtype=jnp.int32))
    return (head_portion.reshape(N_DP * PAIRS_PER_BIN, QUERY_HEADS), query_portion.reshape(N_DP * PAIRS_PER_BIN, QUERY_HEADS), key_value_portion.reshape(N_DP * PAIRS_PER_BIN, KEY_VALUE_HEADS))
```

```python
import functools
import math

import jax
import jax.numpy as jnp
from jax import lax
from jax.experimental import pallas as pl
from jax.experimental.pallas import tpu as pltpu
from jax.sharding import PartitionSpec as P

HEAD_SIZE = 128
PAIRS_PER_BIN = 4
LONGEST_SEGMENT = 128
AXES = ("dp", "head")
SUBLANES = 16
LN2 = math.log(2.0)

TOP_PRECISION = lax.Precision.HIGHEST


bar = lax.optimization_barrier


def split_three(x):
    a1 = x.astype(jnp.bfloat16)
    r = x - a1.astype(jnp.float32)
    a2 = r.astype(jnp.bfloat16)
    a3 = (r - a2.astype(jnp.float32)).astype(jnp.bfloat16)
    return a1, a2, a3


def split_two(x):
    a1 = x.astype(jnp.bfloat16)
    a2 = (x - a1.astype(jnp.float32)).astype(jnp.bfloat16)
    return a1, a2


def nt(a, b):
    return lax.dot_general(
        a, b, (((1,), (1,)), ((), ())), preferred_element_type=jnp.float32
    )


def cat(parts, axis):
    return jnp.concatenate(parts, axis=axis)


def attribution_kernel(
    dims, table, *refs
):
    peers, outer, rows, blocks, groups, slots, bins, window = dims
    br = SUBLANES
    q_hbm = refs[: 3 * peers]
    kv_hbm = refs[3 * peers : 3 * peers + outer]
    seg_ref, start_ref, out_ref = refs[3 * peers + outer : 3 * peers + outer + 3]
    (qbuf, kvbuf, kc_ref, dk_ref, vc_ref, dv_ref, acc_ref, qsem, kvsem) = refs[
        3 * peers + outer + 3 :
    ]
    hs = HEAD_SIZE
    lanes = groups * br

    def kv_copy(t, m, slot):
        return pltpu.make_async_copy(kv_hbm[t].at[m], kvbuf.at[slot], kvsem.at[slot])

    def q_copy(m, a):
        return pltpu.make_async_copy(q_hbm[3 * m + a], qbuf.at[m, a], qsem.at[m, a])

    kv_copy(0, 0, 0).start()
    for m in range(peers):
        for a in range(3):
            q_copy(m, a).start()
    acc_ref[...] = jnp.zeros_like(acc_ref)

    total = outer * peers
    for t in range(outer):

        def split_chunk(m, _, t=t):
            step = t * peers + m
            slot = lax.rem(step, 2)
            kv_copy(t, m, slot).wait()

            @pl.when(m + 1 < peers)
            def _():
                kv_copy(t, m + 1, 1 - slot).start()

            if t + 1 < outer:

                @pl.when(m + 1 == peers)
                def _():
                    kv_copy(t + 1, 0, 1 - slot).start()

            dst = pl.ds(pl.multiple_of(step * rows, rows), rows)
            kc = kvbuf[slot, 0]
            vc = kvbuf[slot, 1]
            dk = kvbuf[slot, 2] - kc
            dv = kvbuf[slot, 3] - vc
            kc_ref[dst, :] = cat(split_three(kc), 1)
            dk_ref[dst, :] = cat(split_three(dk), 1)
            vc_ref[dst, :] = cat(split_two(vc), 1)
            dv_ref[dst, :] = cat(split_two(dv), 1)
            return 0

        lax.fori_loop(0, peers, split_chunk, 0)

    factor = hs**-0.5 / LN2
    row_iota = lax.broadcasted_iota(jnp.int32, (window * br, lanes), 0)
    in_block = lax.rem(lax.broadcasted_iota(jnp.int32, (1, lanes), 1), br)
    pick = lax.broadcasted_iota(jnp.int32, (4 * PAIRS_PER_BIN, lanes), 0)

    def one_block(m, k):
        nb = m * blocks + k
        which_bin = table[nb, 0]
        slot = table[nb, 1]
        first = table[nb, 2]
        here = pl.ds(pl.multiple_of(k * br, br), br)

        def heads(a):
            x = qbuf[m, a, here, :]
            return cat([x[:, h * hs : (h + 1) * hs] for h in range(groups)], 0)

        qc = heads(0)
        dq = (heads(1) - qc) * factor
        qc = qc * factor
        dz = heads(2)
        b1, b2, b3 = split_three(cat([qc, dq], 0))
        z1, z2 = split_two(dz)
        spots = [
            pl.ds(pl.multiple_of(table[nb, 3 + w], br), br) for w in range(window)
        ]
        keys = cat([kc_ref[s, :] for s in spots] + [dk_ref[s, :] for s in spots], 0)
        values = cat([vc_ref[s, :] for s in spots] + [dv_ref[s, :] for s in spots], 0)
        k12 = keys[:, : 2 * hs]
        k13 = cat([keys[:, :hs], keys[:, 2 * hs :]], 1)
        prod = (
            nt(k13, cat([b3, b1], 1))
            + nt(k12, cat([b2, b2], 1))
            + nt(k12, cat([b1, b1], 1))
        )
        vprod = nt(values, cat([cat([z1, z1], 1), cat([z2, z2], 1)], 0))
        wr = window * br
        s_clean = prod[:wr, :lanes]
        t_prod = prod[:wr, lanes:]
        u_prod = prod[wr:, :lanes]
        s_corrupt = (s_clean + t_prod) + (u_prod + prod[wr:, lanes:])
        d_prod = vprod[:wr, :lanes] + vprod[:wr, lanes:]
        e_prod = vprod[wr:, :lanes] + vprod[wr:, lanes:]

        spot = which_bin * slots + slot
        seg = seg_ref[pl.ds(spot, 1), :]
        start = start_ref[pl.ds(spot, 1), :]
        key_pos = row_iota + first * br
        allowed = (key_pos >= start) & (key_pos <= in_block + slot * br)
        s_clean = jnp.where(allowed, s_clean, -1e30)
        s_corrupt = jnp.where(allowed, s_corrupt, -1e30)
        e = jnp.exp2(s_clean - jnp.max(s_clean, axis=0, keepdims=True))
        e2 = jnp.exp2(s_corrupt - jnp.max(s_corrupt, axis=0, keepdims=True))

        def total_of(x):
            return jnp.sum(x, axis=0, keepdims=True)

        norm = total_of(e)
        row_dot = total_of(e * d_prod) / norm
        other = total_of(e2 * (d_prod + e_prod)) / total_of(e2)
        grad = e * (d_prod - row_dot)
        head_term = other - row_dot
        query_term = total_of(grad * t_prod) * LN2 / norm
        kv_term = (total_of(grad * u_prod) * LN2 + total_of(e * e_prod)) / norm
        terms = jnp.where(
            pick < PAIRS_PER_BIN,
            head_term,
            jnp.where(pick < 2 * PAIRS_PER_BIN, query_term, kv_term),
        )
        kept = lax.rem(pick, PAIRS_PER_BIN) == seg
        acc_ref[which_bin] += jnp.where(kept, terms, 0.0)

    def one_peer(m, _):
        for a in range(3):
            pltpu.make_async_copy(q_hbm[a], qbuf.at[m, a], qsem.at[m, a]).wait()

        def body(k, _):
            one_block(m, k)
            return 0

        lax.fori_loop(0, blocks, body, 0)
        return 0

    lax.fori_loop(0, peers, one_peer, 0)

    lane_in = lax.broadcasted_iota(jnp.int32, (lanes, hs), 0)
    lane_out = lax.broadcasted_iota(jnp.int32, (lanes, hs), 1)
    result = jnp.zeros((bins, hs), jnp.float32)
    for r in range(3 * PAIRS_PER_BIN):
        if r < 2 * PAIRS_PER_BIN:
            gather = lane_in // br + r * groups == lane_out
        else:
            gather = lane_out == r - 2 * PAIRS_PER_BIN + 2 * PAIRS_PER_BIN * groups
        result += jnp.dot(
            acc_ref[:, r, :],
            jnp.where(gather, 1.0, 0.0).astype(jnp.float32),
            precision=TOP_PRECISION,
            preferred_element_type=jnp.float32,
        )
    out_ref[...] = result


def attribution(dims, table, q_parts, kv_parts, seg, start):
    peers, outer, rows, blocks, groups, slots, bins, window = dims
    hs = HEAD_SIZE
    lanes = groups * SUBLANES
    total = outer * peers * rows
    f32, bf16 = jnp.float32, jnp.bfloat16
    any_spec = pl.BlockSpec(memory_space=pl.ANY)
    vmem_spec = pl.BlockSpec(memory_space=pltpu.VMEM)
    return pl.pallas_call(
        functools.partial(attribution_kernel, dims),
        out_shape=jax.ShapeDtypeStruct((bins, hs), f32),
        in_specs=[pl.BlockSpec(memory_space=pltpu.SMEM)]
        + [any_spec] * (len(q_parts) + len(kv_parts))
        + [vmem_spec] * 2,
        out_specs=vmem_spec,
        scratch_shapes=[
            pltpu.VMEM((peers, 3, rows, groups * hs), f32),
            pltpu.VMEM((2, 4, rows, hs), f32),
            pltpu.VMEM((total, 3 * hs), bf16),
            pltpu.VMEM((total, 3 * hs), bf16),
            pltpu.VMEM((total, 2 * hs), bf16),
            pltpu.VMEM((total, 2 * hs), bf16),
            pltpu.VMEM((bins, 4 * PAIRS_PER_BIN, lanes), f32),
            pltpu.SemaphoreType.DMA((peers, 3)),
            pltpu.SemaphoreType.DMA((2,)),
        ],
        compiler_params=pltpu.CompilerParams(vmem_limit_bytes=56 << 20),
        name="attribution",
    )(table, *q_parts, *kv_parts, seg, start)


def fast_shards(
    inner,
    query_clean,
    key_clean,
    clean_value_rows,
    query_corrupt,
    key_corrupt,
    corrupted_value_rows,
    cotangent,
    bin_segments,
    plan,
    offsets,
):
    hs = HEAD_SIZE
    dp, heads = lax.axis_size("dp"), lax.axis_size("head")
    outer, peers = dp // inner, inner * heads
    rows, kv_width = key_clean.shape
    groups = query_clean.shape[1] // kv_width
    wide = groups * hs
    slots = offsets.shape[0]
    pack = bin_segments.shape[1]
    br = pack // slots
    blocks = rows // br
    window = min(slots, (LONGEST_SEGMENT - 2) // br + 2)
    own, own_head = lax.axis_index("dp"), lax.axis_index("head")
    depth = own // inner
    mine = own_head * inner + lax.rem(own, inner)

    def place(z, t):
        return (z * inner + t % inner) * heads + t // inner

    def swap(d):
        return [(place(z, t), place(z, t ^ d)) for z in range(outer) for t in range(peers)]

    ring = [(place(z, t), place((z + 1) % outer, t)) for z in range(outer) for t in range(peers)]

    def columns(x, d, width):
        return lax.dynamic_slice_in_dim(x, (mine ^ d) * width, width, axis=1)

    kv = (key_clean, clean_value_rows, key_corrupt, corrupted_value_rows)
    queries = (query_clean, query_corrupt, cotangent)

    def kv_piece(d):
        return jnp.stack([columns(x, d, hs) for x in kv], 0)

    sends = list(range(1, peers))
    kv_here = jnp.stack(
        [kv_piece(0)] + [lax.ppermute(kv_piece(d), AXES, swap(d)) for d in sends], 0
    )
    kv_parts = [kv_here]
    received = {}
    current = kv_here
    steps = max(outer - 1, 1)
    todo = [(d, a) for a in range(3) for d in sends]
    per = -(-len(todo) // steps)
    for step in range(steps):
        batch = todo[step * per : (step + 1) * per]
        parts = [columns(queries[a], d, wide) for d, a in batch]
        current, *parts = bar((current, *parts))
        if outer > 1:
            current = lax.ppermute(current, AXES, ring)
        parts = [lax.ppermute(x, AXES, swap(d)) for x, (d, a) in zip(parts, batch)]
        current, *parts = bar((current, *parts))
        if outer > 1:
            kv_parts.append(current)
        for key, x in zip(batch, parts):
            received[key] = x
    for a in range(3):
        received[(0, a)] = columns(queries[a], 0, wide)
    q_parts = [received[(d, a)] for d in range(peers) for a in range(3)]

    table, seg, start = tables(
        inner, outer, peers, blocks, slots, window, depth, mine, bin_segments, plan, offsets, groups
    )
    dims = (peers, outer, rows, blocks, groups, slots, dp, window)
    partial = attribution(dims, table, q_parts, kv_parts, seg, start)
    arrived = lax.all_to_all(partial, "dp", split_axis=0, concat_axis=0, tiled=True)
    summed = jnp.sum(arrived.reshape(outer, inner, hs), axis=0)
    wide_terms = PAIRS_PER_BIN * groups

    def arrange(x, width):
        x = x.reshape(inner, PAIRS_PER_BIN, width)
        return jnp.transpose(x, (1, 0, 2)).reshape(PAIRS_PER_BIN, inner * width)

    return (
        arrange(summed[:, :wide_terms], groups),
        arrange(summed[:, wide_terms : 2 * wide_terms], groups),
        arrange(summed[:, 2 * wide_terms : 2 * wide_terms + PAIRS_PER_BIN], 1),
    )


def tables(
    inner, outer, peers, blocks, slots, window, depth, mine, bin_segments, plan, offsets, groups
):
    dp = inner * outer
    pack = bin_segments.shape[1]
    br = pack // slots
    i32 = jnp.int32
    meta = lax.all_gather(cat([plan, bin_segments], 1), "dp", axis=0, tiled=True)
    plans, segments = meta[:, :slots], meta[:, slots:]
    count = jnp.arange(slots, dtype=i32)
    device = jnp.arange(dp, dtype=i32)
    filler = jnp.sum(
        jnp.where(plans[:, :, None] == count[None, None, :], count[None, :, None], 0), axis=1
    )
    source = (device[:, None] - offsets[None, :]) % dp
    chosen = jnp.sum(
        jnp.where(source[:, None, :] == device[None, :, None], filler[None, :, :], 0), axis=1
    )
    away = (depth - source // inner) % outer
    peer = ((chosen // blocks) * inner + source % inner) ^ mine
    spots = (((away * peers + peer) * blocks) + chosen % blocks) * br
    other = jnp.arange(peers, dtype=i32) ^ mine
    s_of = depth * inner + other % inner
    block_of = (other // inner)[:, None] * blocks + jnp.arange(blocks, dtype=i32)[None, :]
    hot = (s_of[:, None, None, None] == device[None, None, :, None]) & (
        block_of[:, :, None, None] == count[None, None, None, :]
    )
    slot = jnp.sum(jnp.where(hot, plans[None, None], 0), axis=(2, 3)).reshape(-1)
    distance = jnp.sum(
        jnp.where(slot[:, None] == count[None, :], offsets[None, :], 0), axis=1
    )
    which = (jnp.repeat(s_of, blocks) + distance) % dp
    first = jnp.clip(slot - (window - 1), 0, slots - window)
    wanted = first[:, None] + jnp.arange(window, dtype=i32)[None, :]
    hot_bin = which[:, None] == device[None, :]
    by_bin = jnp.sum(jnp.where(hot_bin[:, :, None], spots[None], 0), axis=1)
    where_keys = jnp.sum(
        jnp.where(wanted[:, :, None] == count[None, None, :], by_bin[:, None, :], 0), axis=2
    )
    table = cat([which[:, None], slot[:, None], first[:, None], where_keys], 1)
    begin = jnp.sum((segments[:, None, :] < segments[:, :, None]).astype(i32), axis=2)

    def lanes(x):
        x = x.reshape(dp * slots, 1, br)
        return jnp.broadcast_to(x, (dp * slots, groups, br)).reshape(dp * slots, groups * br)

    return table, lanes(segments), lanes(begin)


def as_views(query_rows, key_rows, value_rows):
    rows_here = query_rows.shape[0]
    width = key_rows.shape[1] // HEAD_SIZE
    groups = query_rows.shape[1] // key_rows.shape[1]
    return (
        query_rows.reshape(rows_here, width, groups, HEAD_SIZE),
        key_rows.reshape(rows_here, width, HEAD_SIZE),
        value_rows.reshape(rows_here, width, HEAD_SIZE),
    )


def attend(query_matrix, key_collections, value_collection, allowed):
    scale_factor = query_matrix.shape[-1] ** (-0.5)
    score_matrix = (
        jnp.einsum("thxn,whn->hxtw", query_matrix, key_collections, precision=TOP_PRECISION)
        * scale_factor
    )
    score_matrix = jnp.where(allowed, score_matrix, -jnp.inf)
    peak = jnp.max(score_matrix, axis=-1, keepdims=True)
    raised = jnp.exp(score_matrix - peak)
    weight_matrix = raised / jnp.sum(raised, axis=-1, keepdims=True)
    output_tensors = jnp.einsum(
        "whfo,owj->fwhj", weight_matrix, value_collection, precision=TOP_PRECISION
    )
    return (weight_matrix, output_tensors)


def attribute(clean_views, clean_pass, corrupt_views, cotangent, allowed):
    query_matrix, key_collections, value_collection = clean_views
    weight_matrix, output_tensors = clean_pass
    query_other, key_other, value_other = corrupt_views
    scale_factor = query_matrix.shape[-1] ** (-0.5)
    other_outputs = attend(query_other, key_other, value_other, allowed)[1]
    value_gradient = jnp.einsum("xprv,rxpw->vxw", weight_matrix, cotangent, precision=TOP_PRECISION)
    weight_gradient = jnp.einsum(
        "thxn,whn->hxtw", cotangent, value_collection, precision=TOP_PRECISION
    )
    row_dot = jnp.transpose(jnp.sum(cotangent * output_tensors, axis=-1), (1, 2, 0))[..., None]
    score_gradient = weight_matrix * (weight_gradient - row_dot) * scale_factor
    query_gradient = jnp.einsum(
        "whfo,owj->fwhj", score_gradient, key_collections, precision=TOP_PRECISION
    )
    key_gradient = jnp.einsum(
        "xprv,rxpw->vxw", score_gradient, query_matrix, precision=TOP_PRECISION
    )
    head_terms = jnp.sum((other_outputs - output_tensors) * cotangent, axis=-1)
    query_terms = jnp.sum((query_other - query_matrix) * query_gradient, axis=-1)
    kv_terms = jnp.sum(
        (key_other - key_collections) * key_gradient
        + (value_other - value_collection) * value_gradient,
        axis=-1,
    )
    rows_here = query_matrix.shape[0]
    return (head_terms.reshape(rows_here, -1), query_terms.reshape(rows_here, -1), kv_terms)


def causal_mask(segment_ids):
    row_index = jnp.arange(segment_ids.shape[0], dtype=jnp.int32)
    same = segment_ids[:, None] == segment_ids[None, :]
    return jnp.logical_and(same, row_index[:, None] >= row_index[None, :])


def pair_sums(segment_ids, term_sets):
    members = (segment_ids[:, None] == jnp.arange(PAIRS_PER_BIN, dtype=jnp.int32)[None, :]).astype(
        jnp.float32
    )
    return tuple(
        (jnp.dot(members.T, column_set, precision=TOP_PRECISION) for column_set in term_sets)
    )


def send_layout(whole, chosen, block_count):
    blocks = whole.reshape((block_count, -1, whole.shape[1]))
    return jnp.take(blocks, chosen, axis=0).reshape((-1, whole.shape[1]))


def bin_layout(received, sources, devices):
    blocks = received.reshape((devices, -1, received.shape[1]))
    return jnp.take(blocks, sources, axis=0).reshape((-1, received.shape[1]))


def plain_shards(
    query_clean,
    key_clean,
    clean_value_rows,
    query_corrupt,
    key_corrupt,
    corrupted_value_rows,
    cotangent,
    bin_segments,
    plan,
    offsets,
):
    gathered = (
        lax.all_to_all(query_clean, "head", split_axis=1, concat_axis=0, tiled=True),
        lax.all_to_all(key_clean, "head", split_axis=1, concat_axis=0, tiled=True),
        lax.all_to_all(clean_value_rows, "head", split_axis=1, concat_axis=0, tiled=True),
        lax.all_to_all(query_corrupt, "head", split_axis=1, concat_axis=0, tiled=True),
        lax.all_to_all(key_corrupt, "head", split_axis=1, concat_axis=0, tiled=True),
        lax.all_to_all(corrupted_value_rows, "head", split_axis=1, concat_axis=0, tiled=True),
        lax.all_to_all(cotangent, "head", split_axis=1, concat_axis=0, tiled=True),
    )
    devices = lax.axis_size("dp")
    own_index = lax.axis_index("dp")
    block_count = offsets.shape[0]
    distance = jnp.take(offsets, plan[0])
    target = (own_index + distance) % devices
    matches = target[None, :] == jnp.arange(devices, dtype=jnp.int32)[:, None]
    chosen = jnp.sum(
        jnp.where(matches, jnp.arange(block_count, dtype=jnp.int32)[None, :], 0), axis=1
    )
    sources = (own_index - offsets) % devices
    outgoing = [send_layout(array_in, chosen, block_count) for array_in in gathered]
    segment_ids = bin_segments[0]
    allowed = causal_mask(segment_ids)
    arrived = (
        lax.all_to_all(outgoing[0], "dp", split_axis=0, concat_axis=0, tiled=True),
        lax.all_to_all(outgoing[1], "dp", split_axis=0, concat_axis=0, tiled=True),
        lax.all_to_all(outgoing[2], "dp", split_axis=0, concat_axis=0, tiled=True),
        lax.all_to_all(outgoing[3], "dp", split_axis=0, concat_axis=0, tiled=True),
        lax.all_to_all(outgoing[4], "dp", split_axis=0, concat_axis=0, tiled=True),
        lax.all_to_all(outgoing[5], "dp", split_axis=0, concat_axis=0, tiled=True),
        lax.all_to_all(outgoing[6], "dp", split_axis=0, concat_axis=0, tiled=True),
    )
    packed = [bin_layout(array_in, sources, devices) for array_in in arrived]
    clean_views = as_views(packed[0], packed[1], packed[2])
    clean_pass = attend(clean_views[0], clean_views[1], clean_views[2], allowed)
    rest = packed[3:]
    corrupt_views = as_views(rest[0], rest[1], rest[2])
    cot_view = rest[3].reshape(clean_views[0].shape)
    term_sets = attribute(clean_views, clean_pass, corrupt_views, cot_view, allowed)
    head_portion, query_portion, key_value_portion = pair_sums(segment_ids, term_sets)
    return (head_portion, query_portion, key_value_portion)


def solution(mesh):
    dp, heads = mesh.shape["dp"], mesh.shape["head"]

    def shards(*args):
        rows, kv_width = args[1].shape
        kv_heads = kv_width // HEAD_SIZE
        slots, pack = args[9].shape[0], args[7].shape[1]
        groups = args[0].shape[1] // kv_width
        inner = kv_heads // heads
        fits = (
            kv_heads % heads == 0
            and dp % inner == 0
            and kv_heads & (kv_heads - 1) == 0
            and pack // slots == SUBLANES
            and rows % SUBLANES == 0
            and groups * SUBLANES == HEAD_SIZE
            and slots == dp
            and 2 * PAIRS_PER_BIN * groups + PAIRS_PER_BIN <= HEAD_SIZE
            and dp // inner <= 4
        )
        if fits:
            return fast_shards(inner, *args)
        return plain_shards(*args)

    placed = (P(AXES, None),) * 7 + (P("dp", None), P("dp", None), P())
    return jax.shard_map(
        shards,
        mesh=mesh,
        in_specs=placed,
        out_specs=(P("dp", "head"), P("dp", "head"), P("dp", "head")),
        check_vma=False,
    )
```

```python
import functools
import math

import jax
import jax.numpy as jnp
from jax import lax
from jax.experimental import pallas as pl
from jax.experimental.pallas import tpu as pltpu
from jax.sharding import PartitionSpec as P


HEAD_SIZE = 128
PAIRS_PER_BIN = 4
LONGEST_SEGMENT = 128
AXES = ("dp", "head")
SUBLANES = 16
LN2 = math.log(2.0)

TOP_PRECISION = lax.Precision.HIGHEST


META_ROWS = 8
FIRST_QUERIES = 4


def split_three(x):
    a1 = x.astype(jnp.bfloat16)
    r = x - a1.astype(jnp.float32)
    a2 = r.astype(jnp.bfloat16)
    a3 = (r - a2.astype(jnp.float32)).astype(jnp.bfloat16)
    return a1, a2, a3


def split_two(x):
    a1 = x.astype(jnp.bfloat16)
    a2 = (x - a1.astype(jnp.float32)).astype(jnp.bfloat16)
    return a1, a2


def nt(a, b):
    return lax.dot_general(
        a, b, (((1,), (1,)), ((), ())), preferred_element_type=jnp.float32
    )


def cat(parts, axis):
    return jnp.concatenate(parts, axis=axis)


def attribution_kernel(dims, mine, table, *refs):
    peers, outer, rows, blocks, groups, slots, bins, window = dims
    br = SUBLANES
    whole, refs = refs[:3], refs[3:]
    q_hbm, refs = refs[: 3 * (peers - 1)], refs[3 * (peers - 1) :]
    kv_hbm, refs = refs[: outer * peers], refs[outer * peers :]
    seg_ref, start_ref, out_ref, *refs = refs
    (qbuf, kvbuf, kc_ref, dk_ref, vc_ref, dv_ref, *refs) = refs
    (p0, p1, v0, v1, acc_ref, qsem, kvsem) = refs
    slots_of = ((p0, v0), (p1, v1))
    hs = HEAD_SIZE
    lanes = groups * br
    wr = window * br

    for n in range(outer * peers):
        pltpu.make_async_copy(kv_hbm[n], kvbuf.at[n], kvsem.at[n]).start()
    own_columns = pl.ds(pl.multiple_of(mine[0] * groups * hs, groups * hs), groups * hs)
    for a in range(3):
        pltpu.make_async_copy(
            whole[a].at[:, own_columns], qbuf.at[0, a], qsem.at[0, a]
        ).start()
    for m in range(1, peers):
        for a in range(3):
            pltpu.make_async_copy(
                q_hbm[3 * m - 3 + a], qbuf.at[m, a], qsem.at[m, a]
            ).start()
    acc_ref[...] = jnp.zeros_like(acc_ref)

    def split_keys(n, _):
        pltpu.make_async_copy(kv_hbm[0], kvbuf.at[n], kvsem.at[n]).wait()
        dst = pl.ds(pl.multiple_of(n * rows, rows), rows)
        kc = kvbuf[n, :rows, :]
        vc = kvbuf[n, rows : 2 * rows, :]
        dk = kvbuf[n, 2 * rows : 3 * rows, :] - kc
        dv = kvbuf[n, 3 * rows : 4 * rows, :] - vc
        kc_ref[dst, :] = cat(split_three(kc), 1)
        dk_ref[dst, :] = cat(split_three(dk), 1)
        vc_ref[dst, :] = cat(split_two(vc), 1)
        dv_ref[dst, :] = cat(split_two(dv), 1)
        return 0

    lax.fori_loop(0, outer * peers, split_keys, 0)

    factor = hs**-0.5 / LN2
    row_iota = lax.broadcasted_iota(jnp.int32, (wr, lanes), 0)
    in_block = lax.rem(lax.broadcasted_iota(jnp.int32, (1, lanes), 1), br)
    pick = lax.broadcasted_iota(jnp.int32, (4 * PAIRS_PER_BIN, lanes), 0)

    def products(nb, into):
        prod_ref, vprod_ref = into
        m, k = nb // blocks, lax.rem(nb, blocks)
        here = pl.ds(pl.multiple_of(k * br, br), br)

        def heads(a):
            x = qbuf[m, a, here, :]
            return cat([x[:, h * hs : (h + 1) * hs] for h in range(groups)], 0)

        qc = heads(0)
        dq = (heads(1) - qc) * factor
        b1, b2, b3 = split_three(cat([qc * factor, dq], 0))
        z1, z2 = split_two(heads(2))
        spots = [
            pl.ds(pl.multiple_of(table[nb, 3 + w], br), br) for w in range(window)
        ]
        keys = cat([kc_ref[s, :] for s in spots] + [dk_ref[s, :] for s in spots], 0)
        values = cat([vc_ref[s, :] for s in spots] + [dv_ref[s, :] for s in spots], 0)
        k12 = keys[:, : 2 * hs]
        k13 = cat([keys[:, :hs], keys[:, 2 * hs :]], 1)
        prod_ref[...] = (
            nt(k13, cat([b3, b1], 1))
            + nt(k12, cat([b2, b2], 1))
            + nt(k12, cat([b1, b1], 1))
        )
        vprod_ref[...] = nt(values, cat([cat([z1, z1], 1), cat([z2, z2], 1)], 0))

    def total_of(x):
        return jnp.sum(x, axis=0, keepdims=True)

    def reduce(nb, source):
        prod_ref, vprod_ref = source
        which_bin = table[nb, 0]
        slot = table[nb, 1]
        first = table[nb, 2]
        s_clean = prod_ref[:wr, :lanes]
        t_prod = prod_ref[:wr, lanes:]
        u_prod = prod_ref[wr:, :lanes]
        s_corrupt = (s_clean + t_prod) + (u_prod + prod_ref[wr:, lanes:])
        d_prod = vprod_ref[:wr, :lanes] + vprod_ref[:wr, lanes:]
        e_prod = vprod_ref[wr:, :lanes] + vprod_ref[wr:, lanes:]
        spot = which_bin * slots + slot
        seg = seg_ref[pl.ds(spot, 1), :]
        start = start_ref[pl.ds(spot, 1), :]
        key_pos = row_iota + first * br
        allowed = (key_pos >= start) & (key_pos <= in_block + slot * br)
        s_clean = jnp.where(allowed, s_clean, -1e30)
        s_corrupt = jnp.where(allowed, s_corrupt, -1e30)
        e = jnp.exp2(s_clean - jnp.max(s_clean, axis=0, keepdims=True))
        e2 = jnp.exp2(s_corrupt - jnp.max(s_corrupt, axis=0, keepdims=True))
        norm = total_of(e)
        row_dot = total_of(e * d_prod) / norm
        other = total_of(e2 * (d_prod + e_prod)) / total_of(e2)
        grad = e * (d_prod - row_dot)
        head_term = other - row_dot
        query_term = total_of(grad * t_prod) * LN2 / norm
        kv_term = (total_of(grad * u_prod) * LN2 + total_of(e * e_prod)) / norm
        terms = jnp.where(
            pick < PAIRS_PER_BIN,
            head_term,
            jnp.where(pick < 2 * PAIRS_PER_BIN, query_term, kv_term),
        )
        kept = lax.rem(pick, PAIRS_PER_BIN) == seg
        acc_ref[which_bin] += jnp.where(kept, terms, 0.0)

    def wait_peer(m):
        for a in range(3):
            pltpu.make_async_copy(q_hbm[0], qbuf.at[m, a], qsem.at[m, a]).wait()

    last = peers * blocks - 1
    wait_peer(0)
    products(0, slots_of[0])

    def one_peer(m, _):
        @pl.when(m + 1 < peers)
        def _():
            wait_peer(m + 1)

        def pair(j, _):
            nb = m * blocks + 2 * j
            products(nb + 1, slots_of[1])
            reduce(nb, slots_of[0])
            products(jnp.minimum(nb + 2, last), slots_of[0])
            reduce(nb + 1, slots_of[1])
            return 0

        lax.fori_loop(0, blocks // 2, pair, 0)
        return 0

    lax.fori_loop(0, peers, one_peer, 0)

    lane_in = lax.broadcasted_iota(jnp.int32, (lanes, hs), 0)
    lane_out = lax.broadcasted_iota(jnp.int32, (lanes, hs), 1)
    result = jnp.zeros((bins, hs), jnp.float32)
    for r in range(3 * PAIRS_PER_BIN):
        if r < 2 * PAIRS_PER_BIN:
            gather = lane_in // br + r * groups == lane_out
        else:
            gather = lane_out == r - 2 * PAIRS_PER_BIN + 2 * PAIRS_PER_BIN * groups
        result += jnp.dot(
            acc_ref[:, r, :],
            jnp.where(gather, 1.0, 0.0).astype(jnp.float32),
            precision=TOP_PRECISION,
            preferred_element_type=jnp.float32,
        )
    out_ref[...] = result


def attribution(dims, mine, table, whole, q_parts, kv_parts, seg, start):
    peers, outer, rows, _, groups, _, bins, window = dims
    hs = HEAD_SIZE
    lanes = groups * SUBLANES
    wr = window * SUBLANES
    total = outer * peers * rows
    f32, bf16 = jnp.float32, jnp.bfloat16
    any_spec = pl.BlockSpec(memory_space=pl.ANY)
    vmem_spec = pl.BlockSpec(memory_space=pltpu.VMEM)
    parts = (*whole, *q_parts, *kv_parts)
    return pl.pallas_call(
        functools.partial(attribution_kernel, dims),
        out_shape=jax.ShapeDtypeStruct((bins, hs), f32),
        in_specs=[pl.BlockSpec(memory_space=pltpu.SMEM)] * 2
        + [any_spec] * len(parts)
        + [vmem_spec] * 2,
        out_specs=vmem_spec,
        scratch_shapes=[
            pltpu.VMEM((peers, 3, rows, groups * hs), f32),
            pltpu.VMEM((outer * peers, *kv_parts[0].shape), f32),
            pltpu.VMEM((total, 3 * hs), bf16),
            pltpu.VMEM((total, 3 * hs), bf16),
            pltpu.VMEM((total, 2 * hs), bf16),
            pltpu.VMEM((total, 2 * hs), bf16),
            pltpu.VMEM((2 * wr, 2 * lanes), f32),
            pltpu.VMEM((2 * wr, 2 * lanes), f32),
            pltpu.VMEM((2 * wr, 2 * lanes), f32),
            pltpu.VMEM((2 * wr, 2 * lanes), f32),
            pltpu.VMEM((bins, 4 * PAIRS_PER_BIN, lanes), f32),
            pltpu.SemaphoreType.DMA((peers, 3)),
            pltpu.SemaphoreType.DMA((outer * peers,)),
        ],
        compiler_params=pltpu.CompilerParams(vmem_limit_bytes=56 << 20),
        name="attribution",
    )(mine.reshape(1), table, *parts, seg, start)


def pack_kernel(peers, rows, mine, key_clean, value_clean, key_corrupt, value_corrupt, tile, *outs):
    hs = HEAD_SIZE
    for d in range(peers):
        columns = pl.ds(pl.multiple_of((mine[0] ^ d) * hs, hs), hs)
        for a, x in enumerate((key_clean, value_clean, key_corrupt, value_corrupt)):
            outs[d][a * rows : (a + 1) * rows, :] = x[:, columns]
        outs[d][4 * rows :, :] = tile[...]


def pack(peers, mine, kv, tile):
    rows = kv[0].shape[0]
    vmem_spec = pl.BlockSpec(memory_space=pltpu.VMEM)
    return pl.pallas_call(
        functools.partial(pack_kernel, peers, rows),
        out_shape=[
            jax.ShapeDtypeStruct((4 * rows + META_ROWS, HEAD_SIZE), jnp.float32)
        ] * peers,
        in_specs=[pl.BlockSpec(memory_space=pltpu.SMEM)] + [vmem_spec] * 5,
        out_specs=[vmem_spec] * peers,
        name="pack",
    )(mine.reshape(1), *kv, tile)


def collect_kernel(first, *refs):
    parts, out_ref, sem = refs[:-2], refs[-2], refs[-1]
    copies = [
        pltpu.make_async_copy(x.at[first:, :], out_ref.at[n], sem.at[n])
        for n, x in enumerate(parts)
    ]
    for copy in copies:
        copy.start()
    for copy in copies:
        copy.wait()


def collect(first, parts):
    count = len(parts)
    return pl.pallas_call(
        functools.partial(collect_kernel, first),
        out_shape=jax.ShapeDtypeStruct((count, META_ROWS, HEAD_SIZE), jnp.float32),
        in_specs=[pl.BlockSpec(memory_space=pl.ANY)] * count,
        out_specs=pl.BlockSpec(memory_space=pltpu.VMEM),
        scratch_shapes=[pltpu.SemaphoreType.DMA((count,))],
        name="collect",
    )(*parts)


def send_order(peers):
    half = peers // 2
    low = [d for d in range(2, half)]
    high = [d for d in range(half, peers) if not d & (half - 1) & ~1]
    across = [d for d in range(half, peers) if d not in high]
    turns = [d for pair in zip(low, high) for d in pair]
    rest = [d for d in range(2, peers) if d not in turns and d not in across]
    return [1] + turns + rest + across


def query_order(peers):
    order = send_order(peers)
    pieces = []
    for n in range(1, len(order), 2):
        pieces += [(d, a) for a in range(3) for d in order[n : n + 2]]
    return pieces + [(order[0], a) for a in range(3)]


def fast_shards(
    inner,
    query_clean,
    key_clean,
    clean_value_rows,
    query_corrupt,
    key_corrupt,
    corrupted_value_rows,
    cotangent,
    bin_segments,
    plan,
    offsets,
):
    hs = HEAD_SIZE
    dp, heads = lax.axis_size("dp"), lax.axis_size("head")
    outer, peers = dp // inner, inner * heads
    rows, kv_width = key_clean.shape
    groups = query_clean.shape[1] // kv_width
    wide = groups * hs
    slots = offsets.shape[0]
    pack_rows = bin_segments.shape[1]
    br = pack_rows // slots
    blocks = rows // br
    window = min(slots, (LONGEST_SEGMENT - 2) // br + 2)
    own, own_head = lax.axis_index("dp"), lax.axis_index("head")
    depth = own // inner
    mine = own_head * inner + lax.rem(own, inner)

    def place(z, t):
        return (z * inner + t % inner) * heads + t // inner

    def swap(d):
        return [(place(z, t), place(z, t ^ d)) for z in range(outer) for t in range(peers)]

    ring = [(place(z, t), place((z + 1) % outer, t)) for z in range(outer) for t in range(peers)]

    meta = cat([plan, bin_segments], 1)[0].astype(jnp.float32)
    tile = jnp.pad(meta, (0, META_ROWS * hs - slots - pack_rows)).reshape(META_ROWS, hs)
    queries = (query_clean, query_corrupt, cotangent)
    order = [0] + send_order(peers)

    def send(x, perm):
        return lax.ppermute(x, AXES, perm)

    kv = (key_clean, clean_value_rows, key_corrupt, corrupted_value_rows)
    out = pack(peers, mine, kv, tile)
    here = [out[0]] + [send(out[d], swap(d)) for d in range(1, peers)]
    levels = [here]
    for _ in range(1, outer):
        levels.append([send(levels[-1][d], ring) for d in range(peers)])

    pieces = query_order(peers)
    received = {}
    cuts = [(0, FIRST_QUERIES), (FIRST_QUERIES, 10), (10, 16), (16, len(pieces))]
    for n, (low, high) in enumerate(cuts):
        index = mine
        if n:
            d = order[n - 1]
            index, levels[1][d] = lax.optimization_barrier((mine, levels[1][d]))
        for d, a in pieces[low:high]:
            cut = lax.dynamic_slice_in_dim(queries[a], (index ^ d) * wide, wide, axis=1)
            received[d, a] = send(cut, swap(d))
    q_parts = [received[d, a] for d in order[1:] for a in range(3)]
    kv_parts = [x for level in levels for x in level]

    collected = collect(4 * rows, [level[d] for level in levels for d in range(inner)])
    table, seg, start = tables(
        inner, outer, peers, blocks, slots, pack_rows, window, depth, mine, own_head,
        order, collected.reshape(outer * inner, -1), offsets, groups,
    )
    dims = (peers, outer, rows, blocks, groups, slots, dp, window)
    partial = attribution(dims, mine, table, queries, q_parts, kv_parts, seg, start)
    arrived = lax.all_to_all(partial, "dp", split_axis=0, concat_axis=0, tiled=True)
    summed = jnp.sum(arrived.reshape(outer, inner, hs), axis=0)
    wide_terms = PAIRS_PER_BIN * groups

    def arrange(x, width):
        x = x.reshape(inner, PAIRS_PER_BIN, width)
        return jnp.transpose(x, (1, 0, 2)).reshape(PAIRS_PER_BIN, inner * width)

    return (
        arrange(summed[:, :wide_terms], groups),
        arrange(summed[:, wide_terms : 2 * wide_terms], groups),
        arrange(summed[:, 2 * wide_terms : 2 * wide_terms + PAIRS_PER_BIN], 1),
    )


def tables(
    inner, outer, peers, blocks, slots, pack, window, depth, mine, own_head,
    arrival, collected, offsets, groups,
):
    dp = inner * outer
    br = pack // slots
    i32 = jnp.int32
    every = jnp.arange(dp, dtype=i32)
    came = ((depth - every // inner) % outer) * inner
    came = came + (mine ^ (own_head * inner + every % inner))
    meta = jnp.take(collected, came, axis=0).astype(i32)
    plans, segments = meta[:, :slots], meta[:, slots : slots + pack]
    count = jnp.arange(slots, dtype=i32)
    device = jnp.arange(dp, dtype=i32)
    filler = jnp.sum(
        jnp.where(plans[:, :, None] == count[None, None, :], count[None, :, None], 0), axis=1
    )
    source = (device[:, None] - offsets[None, :]) % dp
    chosen = jnp.sum(
        jnp.where(source[:, None, :] == device[None, :, None], filler[None, :, :], 0), axis=1
    )
    away = (depth - source // inner) % outer
    peer = ((chosen // blocks) * inner + source % inner) ^ mine
    spots = (((away * peers + peer) * blocks) + chosen % blocks) * br
    other = jnp.array(arrival, i32) ^ mine
    s_of = depth * inner + other % inner
    block_of = (other // inner)[:, None] * blocks + jnp.arange(blocks, dtype=i32)[None, :]
    hot = (s_of[:, None, None, None] == device[None, None, :, None]) & (
        block_of[:, :, None, None] == count[None, None, None, :]
    )
    slot = jnp.sum(jnp.where(hot, plans[None, None], 0), axis=(2, 3)).reshape(-1)
    distance = jnp.sum(
        jnp.where(slot[:, None] == count[None, :], offsets[None, :], 0), axis=1
    )
    which = (jnp.repeat(s_of, blocks) + distance) % dp
    first = jnp.clip(slot - (window - 1), 0, slots - window)
    wanted = first[:, None] + jnp.arange(window, dtype=i32)[None, :]
    hot_bin = which[:, None] == device[None, :]
    by_bin = jnp.sum(jnp.where(hot_bin[:, :, None], spots[None], 0), axis=1)
    where_keys = jnp.sum(
        jnp.where(wanted[:, :, None] == count[None, None, :], by_bin[:, None, :], 0), axis=2
    )
    table = cat([which[:, None], slot[:, None], first[:, None], where_keys], 1)
    begin = jnp.sum((segments[:, None, :] < segments[:, :, None]).astype(i32), axis=2)

    def lanes(x):
        x = x.reshape(dp * slots, 1, br)
        return jnp.broadcast_to(x, (dp * slots, groups, br)).reshape(dp * slots, groups * br)

    return table, lanes(segments), lanes(begin)


def as_views(query_rows, key_rows, value_rows):
    rows_here = query_rows.shape[0]
    width = key_rows.shape[1] // HEAD_SIZE
    groups = query_rows.shape[1] // key_rows.shape[1]
    return (
        query_rows.reshape(rows_here, width, groups, HEAD_SIZE),
        key_rows.reshape(rows_here, width, HEAD_SIZE),
        value_rows.reshape(rows_here, width, HEAD_SIZE),
    )


def attend(query_matrix, key_collections, value_collection, allowed):
    scale_factor = query_matrix.shape[-1] ** (-0.5)
    score_matrix = (
        jnp.einsum("thxn,whn->hxtw", query_matrix, key_collections, precision=TOP_PRECISION)
        * scale_factor
    )
    score_matrix = jnp.where(allowed, score_matrix, -jnp.inf)
    peak = jnp.max(score_matrix, axis=-1, keepdims=True)
    raised = jnp.exp(score_matrix - peak)
    weight_matrix = raised / jnp.sum(raised, axis=-1, keepdims=True)
    output_tensors = jnp.einsum(
        "whfo,owj->fwhj", weight_matrix, value_collection, precision=TOP_PRECISION
    )
    return (weight_matrix, output_tensors)


def attribute(clean_views, clean_pass, corrupt_views, cotangent, allowed):
    query_matrix, key_collections, value_collection = clean_views
    weight_matrix, output_tensors = clean_pass
    query_other, key_other, value_other = corrupt_views
    scale_factor = query_matrix.shape[-1] ** (-0.5)
    other_outputs = attend(query_other, key_other, value_other, allowed)[1]
    value_gradient = jnp.einsum("xprv,rxpw->vxw", weight_matrix, cotangent, precision=TOP_PRECISION)
    weight_gradient = jnp.einsum(
        "thxn,whn->hxtw", cotangent, value_collection, precision=TOP_PRECISION
    )
    row_dot = jnp.transpose(jnp.sum(cotangent * output_tensors, axis=-1), (1, 2, 0))[..., None]
    score_gradient = weight_matrix * (weight_gradient - row_dot) * scale_factor
    query_gradient = jnp.einsum(
        "whfo,owj->fwhj", score_gradient, key_collections, precision=TOP_PRECISION
    )
    key_gradient = jnp.einsum(
        "xprv,rxpw->vxw", score_gradient, query_matrix, precision=TOP_PRECISION
    )
    head_terms = jnp.sum((other_outputs - output_tensors) * cotangent, axis=-1)
    query_terms = jnp.sum((query_other - query_matrix) * query_gradient, axis=-1)
    kv_terms = jnp.sum(
        (key_other - key_collections) * key_gradient
        + (value_other - value_collection) * value_gradient,
        axis=-1,
    )
    rows_here = query_matrix.shape[0]
    return (head_terms.reshape(rows_here, -1), query_terms.reshape(rows_here, -1), kv_terms)


def causal_mask(segment_ids):
    row_index = jnp.arange(segment_ids.shape[0], dtype=jnp.int32)
    same = segment_ids[:, None] == segment_ids[None, :]
    return jnp.logical_and(same, row_index[:, None] >= row_index[None, :])


def pair_sums(segment_ids, term_sets):
    members = (segment_ids[:, None] == jnp.arange(PAIRS_PER_BIN, dtype=jnp.int32)[None, :]).astype(
        jnp.float32
    )
    return tuple(
        (jnp.dot(members.T, column_set, precision=TOP_PRECISION) for column_set in term_sets)
    )


def send_layout(whole, chosen, block_count):
    blocks = whole.reshape((block_count, -1, whole.shape[1]))
    return jnp.take(blocks, chosen, axis=0).reshape((-1, whole.shape[1]))


def bin_layout(received, sources, devices):
    blocks = received.reshape((devices, -1, received.shape[1]))
    return jnp.take(blocks, sources, axis=0).reshape((-1, received.shape[1]))


def plain_shards(
    query_clean,
    key_clean,
    clean_value_rows,
    query_corrupt,
    key_corrupt,
    corrupted_value_rows,
    cotangent,
    bin_segments,
    plan,
    offsets,
):
    gathered = (
        lax.all_to_all(query_clean, "head", split_axis=1, concat_axis=0, tiled=True),
        lax.all_to_all(key_clean, "head", split_axis=1, concat_axis=0, tiled=True),
        lax.all_to_all(clean_value_rows, "head", split_axis=1, concat_axis=0, tiled=True),
        lax.all_to_all(query_corrupt, "head", split_axis=1, concat_axis=0, tiled=True),
        lax.all_to_all(key_corrupt, "head", split_axis=1, concat_axis=0, tiled=True),
        lax.all_to_all(corrupted_value_rows, "head", split_axis=1, concat_axis=0, tiled=True),
        lax.all_to_all(cotangent, "head", split_axis=1, concat_axis=0, tiled=True),
    )
    devices = lax.axis_size("dp")
    own_index = lax.axis_index("dp")
    block_count = offsets.shape[0]
    distance = jnp.take(offsets, plan[0])
    target = (own_index + distance) % devices
    matches = target[None, :] == jnp.arange(devices, dtype=jnp.int32)[:, None]
    chosen = jnp.sum(
        jnp.where(matches, jnp.arange(block_count, dtype=jnp.int32)[None, :], 0), axis=1
    )
    sources = (own_index - offsets) % devices
    outgoing = [send_layout(array_in, chosen, block_count) for array_in in gathered]
    segment_ids = bin_segments[0]
    allowed = causal_mask(segment_ids)
    arrived = (
        lax.all_to_all(outgoing[0], "dp", split_axis=0, concat_axis=0, tiled=True),
        lax.all_to_all(outgoing[1], "dp", split_axis=0, concat_axis=0, tiled=True),
        lax.all_to_all(outgoing[2], "dp", split_axis=0, concat_axis=0, tiled=True),
        lax.all_to_all(outgoing[3], "dp", split_axis=0, concat_axis=0, tiled=True),
        lax.all_to_all(outgoing[4], "dp", split_axis=0, concat_axis=0, tiled=True),
        lax.all_to_all(outgoing[5], "dp", split_axis=0, concat_axis=0, tiled=True),
        lax.all_to_all(outgoing[6], "dp", split_axis=0, concat_axis=0, tiled=True),
    )
    packed = [bin_layout(array_in, sources, devices) for array_in in arrived]
    clean_views = as_views(packed[0], packed[1], packed[2])
    clean_pass = attend(clean_views[0], clean_views[1], clean_views[2], allowed)
    rest = packed[3:]
    corrupt_views = as_views(rest[0], rest[1], rest[2])
    cot_view = rest[3].reshape(clean_views[0].shape)
    term_sets = attribute(clean_views, clean_pass, corrupt_views, cot_view, allowed)
    head_portion, query_portion, key_value_portion = pair_sums(segment_ids, term_sets)
    return (head_portion, query_portion, key_value_portion)


def solution(mesh):
    dp, heads = mesh.shape["dp"], mesh.shape["head"]
    placed = (P(AXES, None),) * 7 + (P("dp", None), P("dp", None), P())

    def fast_inner(shapes):
        rows, kv_width = shapes[1][0] // (dp * heads), shapes[1][1]
        kv_heads = kv_width // HEAD_SIZE
        slots, pack = shapes[9][0], shapes[7][1]
        groups = shapes[0][1] // kv_width
        inner = kv_heads // heads
        fits = (
            kv_heads == inner * heads
            and dp % inner == 0
            and 1 < dp // inner <= 4
            and kv_heads & (kv_heads - 1) == 0
            and pack // slots == SUBLANES
            and rows % (2 * SUBLANES) == 0
            and groups * SUBLANES == HEAD_SIZE
            and slots == dp
            and slots + pack <= META_ROWS * HEAD_SIZE
            and 2 * PAIRS_PER_BIN * groups + PAIRS_PER_BIN <= HEAD_SIZE
        )
        return inner if fits else 0

    def run(*args):
        inner = fast_inner([x.shape for x in args])

        def shards(*parts):
            if not inner:
                return plain_shards(*parts)
            return fast_shards(inner, *parts)

        step = jax.shard_map(
            shards,
            mesh=mesh,
            in_specs=placed,
            out_specs=(P("dp", "head"),) * 3,
            check_vma=False,
        )
        return step(*args)

    return run
```
